32 devices in a mesh: tp: 4 (over z), ep: 8 (over y, x, core).
Axes of the slice: x: 2, y: 2, z: 4, core: 2. Of those that a mesh axis runs over, the one named last changes fastest.
Arguments:
- tokens: bfloat16 [3072, 2048], P('ep', 'tp'), may hold values from -6 to 6
- norm_gain: float32 [2048], replicated, may hold values from 0.25 to 1.75
- shared_gate: bfloat16 [2048, 2816], P('ep', 'tp'), may hold values from -0.125 to 0.125
- shared_up: bfloat16 [2048, 2816], P('ep', 'tp'), may hold values from -0.125 to 0.125
- shared_down: bfloat16 [2816, 2048], P('tp', 'ep'), may hold values from -0.15625 to 0.15625
- expert_gate: bfloat16 [4, 8, 704, 2048], P('tp', 'ep'), may hold values from -0.125 to 0.125
- expert_up: bfloat16 [4, 8, 704, 2048], P('tp', 'ep'), may hold values from -0.125 to 0.125
- expert_down: bfloat16 [16, 1408, 2048], P('ep', None, 'tp'), may hold values from -0.15625 to 0.15625
- chosen: int32 [16, 384], P('ep'), may hold values from 0 to 3071, as said below
- gates: float32 [16, 384], P('ep'), may hold values from 0.1 to 1
Outputs:
- mixed: bfloat16 [3072, 2048], P('ep', 'tp')
The draws below stay inside these ranges and needn't reach their ends.
Inputs may be any that keep to these rules, and one draw needn't show every extreme that they name: Each row of chosen holds 384 different token indices in rising order. Of one row, at most 96 lie among the 384 tokens of one index of ep (tokens s * 384 to (s + 1) * 384 - 1), and in every row exactly 96 lie among those of some index.
All inputs are finite; a program needn't handle non-finite values.
Results may differ from the reference program's by a relative error of at most 0.012.
Values may be sent and summed in bfloat16 or wider, within the bound.
No kernel may reach another device: no remote copies, remote signals or barrier semaphores. Data moves between devices by JAX's collectives and lax.ppermute only.
A program may use at most 64 MiB of HBM per device.

```python
import jax
import jax.numpy as jnp
from jax import lax

D = 2048
FS = 2816
F = 1408
EXP_DEV = 2
TOK_DEV = 384
TOKENS = 3072
EXPERTS = 16
SPLIT = 2
CAP = 384
N_TP = 4
N_EP = 8


def expert_choices(expert_key):
    key_pair, key_shift, key_rank = jax.random.split(expert_key, 3)
    halves = N_EP // 2
    average = CAP // N_EP
    pairing = jax.random.permutation(key_pair, N_EP)
    shifts = jax.random.randint(key_shift, (halves,), 0, average + 1).astype(jnp.int32)
    shifts = shifts.at[0].set(average)
    counts = jnp.full((N_EP,), average, jnp.int32)
    counts = counts.at[pairing[:halves]].add(shifts).at[pairing[halves:]].add(-shifts)
    rank_keys = jax.random.split(key_rank, N_EP)
    rankings = jax.vmap(source_ranking)(rank_keys)
    flags = (rankings < counts[:, None]).reshape(-1).astype(jnp.int32)
    places = jnp.cumsum(flags) - 1
    places = jnp.where(flags > 0, places, CAP)
    token_ids = jnp.arange(N_EP * TOK_DEV, dtype=jnp.int32)
    return jnp.zeros((CAP,), jnp.int32).at[places].set(token_ids, mode='drop')


def source_ranking(rank_key):
    return jax.random.permutation(rank_key, TOK_DEV).astype(jnp.int32)


def draw_chosen(key, part):
    expert_keys = jax.random.split(jax.random.fold_in(key, 11), EXPERTS)
    return jax.vmap(expert_choices)(expert_keys)


def strengthened(array, own_key, source, target, shards_of, factor):
    owner, partner = [(jnp.arange(array.shape[position]) // (array.shape[position] // shards_of)).reshape([-1 if axis == position else 1 for axis in range(array.ndim)]) for position in (source, target)]
    chosen = jax.random.permutation(own_key, shards_of)[partner]
    strong = (owner == chosen) | (owner == (partner + shards_of // 2) % shards_of)
    return jnp.where(strong, factor * array, array)


def levels(stream_key, dims, cuts, low, top_value):
    def one(axis_at, shards_of):
        draws = jax.random.uniform(jax.random.fold_in(jax.random.fold_in(stream_key, 6), axis_at), (shards_of,), jnp.float32, low / len(cuts), top_value / len(cuts))
        return jnp.repeat(jnp.exp(draws), dims[axis_at] // shards_of).reshape((-1,) + (1,) * (len(dims) - axis_at - 1))

    level = one(*cuts[0])
    for cut in cuts[1:]:
        level = level * one(*cut)
    return level


def normal_values(key, shape, scale, most, cuts=(), held_as=jnp.bfloat16):
    entries = jax.random.normal(key, shape, jnp.float32) * scale
    if len(cuts) > 0:
        entries = levels(key, shape, cuts, -0.22, 0.18) * entries
    return jnp.clip(entries, min=-most, max=most).astype(held_as)


def bell_draw_with(own_key, extent, scale, reach, cuts, heavy, held_as=jnp.bfloat16):
    entries = scale * jax.random.normal(own_key, extent, jnp.float32)
    if cuts:
        entries = entries * levels(own_key, extent, cuts, -0.22, 0.18)
    return jnp.clip(strengthened(entries, jax.random.fold_in(own_key, 3), *heavy), -reach, reach).astype(held_as)


def setup_inputs(seed: int = 0) -> dict:
    key_list = jax.random.split(jax.random.key(seed), 11)
    tokens = normal_values(key_list[0], (TOKENS, D), 1.0, 6.0, ((0, 8), (1, 4)))
    norm_gain = jnp.clip(1.0 + 0.15 * jax.random.normal(key_list[1], (D,), jnp.float32), 0.25, 1.75)
    shared_gate = normal_values(key_list[2], (D, FS), D ** -0.5, 0.125, ((0, 8), (1, 4)))
    shared_up = normal_values(key_list[3], (D, FS), D ** -0.5, 0.125, ((0, 8), (1, 4)))
    shared_down = bell_draw_with(key_list[4], (FS, D), FS ** -0.5, 0.15625, ((0, 4), (1, 8)), (0, 1, 8, 2.0))
    expert_gate = normal_values(key_list[5], (N_TP, N_EP, F // SPLIT, D), D ** -0.5, 0.125, ((0, 4), (1, 8)))
    expert_up = normal_values(key_list[6], (N_TP, N_EP, F // SPLIT, D), D ** -0.5, 0.125, ((0, 4), (1, 8)))
    expert_down = normal_values(key_list[7], (EXPERTS, F, D), F ** -0.5, 0.15625, ((0, 8), (2, 4)))
    chosen = draw_chosen(jax.random.fold_in(key_list[10], 71), 0)
    gates = jnp.clip(0.1 + 0.9 * jax.random.uniform(key_list[9], (EXPERTS, CAP), jnp.float32) ** levels(key_list[9], (EXPERTS, CAP), ((0, 8),), -0.2, 0.2), 0.1, 1.0)
    return dict(tokens=tokens, norm_gain=norm_gain, shared_gate=shared_gate, shared_up=shared_up, shared_down=shared_down, expert_gate=expert_gate, expert_up=expert_up, expert_down=expert_down, chosen=chosen, gates=gates)


norm_eps = 1e-06

def reference(tokens, norm_gain, shared_gate, shared_up, shared_down, expert_gate, expert_up, expert_down, chosen, gates):
    widened = tokens.astype(jnp.float32)
    inv_scale = lax.rsqrt(lax.optimization_barrier(jnp.mean(widened * widened, axis=1, keepdims=True)) + norm_eps)
    normed = (widened * inv_scale * norm_gain.astype(jnp.float32)).astype(jnp.bfloat16)
    gate_sum = jnp.dot(normed, shared_gate, preferred_element_type=jnp.float32)
    up_sum = jnp.dot(normed, shared_up, preferred_element_type=jnp.float32)
    shared_hidden = (jax.nn.silu(gate_sum) * up_sum).astype(jnp.bfloat16)
    shared_out = jnp.dot(shared_hidden, shared_down, preferred_element_type=jnp.float32)
    split_count = N_TP // EXP_DEV

    def expert_term(expert_index):
        ep_column = (expert_index // EXP_DEV).astype(jnp.int32)
        expert_slot = (expert_index % EXP_DEV).astype(jnp.int32)

        def weight_of(weights):
            picked = lax.dynamic_index_in_dim(weights, ep_column, 1, keepdims=False)
            picked = lax.dynamic_slice_in_dim(picked, expert_slot * split_count, split_count, 0)
            return jnp.transpose(picked.reshape(F, D))
        token_ids = lax.dynamic_index_in_dim(chosen, expert_index, 0, keepdims=False)
        token_rows = jnp.take(normed, token_ids, axis=0)
        gate_values = jnp.dot(token_rows, weight_of(expert_gate), preferred_element_type=jnp.float32)
        up_values = jnp.dot(token_rows, weight_of(expert_up), preferred_element_type=jnp.float32)
        hidden = (jax.nn.silu(gate_values) * up_values).astype(jnp.bfloat16)
        down_weight = lax.dynamic_index_in_dim(expert_down, expert_index, 0, keepdims=False)
        outputs = jnp.dot(hidden, down_weight, preferred_element_type=jnp.float32)
        gate_row = lax.dynamic_index_in_dim(gates, expert_index, 0, keepdims=False).astype(jnp.float32)
        return (gate_row[:, None] * outputs).astype(jnp.bfloat16)
    weighted = lax.map(expert_term, jnp.arange(EXPERTS, dtype=jnp.int32))
    routed = jnp.zeros((TOKENS, D), jnp.float32).at[chosen.reshape(-1)].add(weighted.reshape(-1, D).astype(jnp.float32))
    return (shared_out + routed).astype(jnp.bfloat16)
```

```python
import jax
import jax.numpy as jnp
from jax import lax
from jax.experimental import pallas as pl
from jax.experimental.pallas import tpu as pltpu
from jax.sharding import PartitionSpec as P

norm_eps = 1e-06
F32 = jnp.float32
BF16 = jnp.bfloat16


HBM_SPEC = pl.BlockSpec(memory_space=pltpu.HBM)
VMEM_SPEC = pl.BlockSpec(memory_space=pltpu.VMEM)
SMEM_SPEC = pl.BlockSpec(memory_space=pltpu.SMEM)


def swap(x, axis, mask):
    count = lax.axis_size(axis)
    return lax.ppermute(x, axis, [(i, i ^ mask) for i in range(count)])


def line_gather(near, far, axis):
    pair = lax.ppermute(near, axis, [(0, 1), (1, 0), (2, 3), (3, 2)])
    middle = lax.ppermute(far, axis, [(1, 2), (2, 1)])
    ends = lax.ppermute(far, axis, [(0, 2), (3, 1)])
    relay_middle = lax.ppermute(middle, axis, [(2, 3), (1, 0)])
    relay_ends = lax.ppermute(ends, axis, [(2, 3), (1, 0)])
    return [
        ([near], 0),
        ([pair], 1),
        ([ends, relay_middle], 2),
        ([middle, relay_ends], 3),
    ]


def box_gather(x, axis):
    half = x.shape[0] // 2
    across = swap(x, axis, 2)
    along = swap(x, axis, 4)
    low = swap(along[:half], axis, 2)
    high = swap(across[half:], axis, 4)
    pieces = [(x, 0, 0), (across, 2, 0), (along, 4, 0), (low, 6, 0), (high, 6, 1)]
    return pieces + [(swap(a, axis, 1), m ^ 1, h) for a, m, h in pieces]


def start_copies(pieces, refs, pos_ref, flag, target, sems, first):
    waits = []
    at = 0
    for number, (count, shape, row_slot, col_slot) in enumerate(pieces):
        row = 0 if row_slot is None else pl.multiple_of(pos_ref[row_slot], 16)
        col = 0 if col_slot is None else pl.multiple_of(pos_ref[col_slot], 128)
        dst = target.at[pl.ds(row, shape[0]), pl.ds(col, shape[1])]
        sem = sems.at[first + number]
        if count == 1:
            pltpu.make_async_copy(refs[at], dst, sem).start()
        else:
            one, two = refs[at], refs[at + 1]

            @pl.when(flag != 0)
            def _(one=one, dst=dst, sem=sem):
                pltpu.make_async_copy(one, dst, sem).start()

            @pl.when(flag == 0)
            def _(two=two, dst=dst, sem=sem):
                pltpu.make_async_copy(two, dst, sem).start()

        waits.append(pltpu.make_async_copy(refs[at], dst, sem))
        at += count
    return waits


class Layout:
    def __init__(self, flag):
        self.arrays = []
        self.slots = [flag]
        self.lists = []

    def add(self, pieces):
        entries = []
        for arrays, row, col in pieces:
            slots = []
            for value in (row, col):
                if value is None:
                    slots.append(None)
                else:
                    slots.append(len(self.slots))
                    self.slots.append(value)
            entries.append((len(arrays), arrays[0].shape, slots[0], slots[1]))
            self.arrays.extend(arrays)
        self.lists.append(entries)

    def positions(self):
        return jnp.stack([jnp.asarray(v, jnp.int32) for v in self.slots])

    def split(self, refs):
        out = []
        at = 0
        for entries in self.lists:
            size = sum(e[0] for e in entries)
            out.append(refs[at : at + size])
            at += size
        return out

    def count(self):
        return sum(len(e) for e in self.lists)


def silu(v):
    return v / (1.0 + jnp.exp(-v))


def normalise(x_ref, gain_ref):
    wide = x_ref[...].astype(F32)
    scale = lax.rsqrt(jnp.mean(wide * wide, axis=1, keepdims=True) + norm_eps)
    x_ref[...] = (wide * scale * gain_ref[...]).astype(BF16)


def dot(a, b, dims):
    return lax.dot_general(a, b, (dims, ((), ())), preferred_element_type=F32)


def gather_rows(token_pieces, flag, chosen_columns, total, cap):
    experts = chosen_columns.shape[0] // cap
    width = token_pieces[0][0][0].shape[1]
    layout = Layout(flag)
    layout.add(token_pieces)

    def body(pos_ref, chosen_ref, *refs):
        ins = refs[: len(layout.arrays)]
        outs = refs[len(layout.arrays) : len(layout.arrays) + experts]
        tokens_ref, sems = refs[len(layout.arrays) + experts :]
        (token_refs,) = layout.split(ins)
        waits = start_copies(
            layout.lists[0], token_refs, pos_ref, pos_ref[0], tokens_ref, sems, 0
        )
        for w in waits:
            w.wait()
        block = min(total, 3072)
        for expert in range(experts):
            ids = chosen_ref[expert * cap : (expert + 1) * cap, :]
            acc = None
            for start in range(0, total, block):
                span = lax.broadcasted_iota(jnp.int32, (cap, block), 1) + start
                picker = jnp.where(ids == span, 1.0, 0.0).astype(BF16)
                part = dot(picker, tokens_ref[start : start + block, :], ((1,), (0,)))
                acc = part if acc is None else acc + part
            outs[expert][...] = acc.astype(BF16)

    return pl.pallas_call(
        body,
        out_shape=[jax.ShapeDtypeStruct((cap, width), BF16)] * experts,
        in_specs=[SMEM_SPEC, VMEM_SPEC] + [HBM_SPEC] * len(layout.arrays),
        out_specs=[VMEM_SPEC] * experts,
        scratch_shapes=[
            pltpu.VMEM((total, width), BF16),
            pltpu.SemaphoreType.DMA((layout.count(),)),
        ],
        name="gather_rows",
    )(layout.positions(), chosen_columns, *layout.arrays)


def expert_hidden(row_pieces, flag, gain, gate, up):
    hidden, features = gate.shape
    cap = row_pieces[0][0][0].shape[0]
    layout = Layout(flag)
    layout.add(row_pieces)

    def body(pos_ref, gain_ref, gate_hbm, up_hbm, *refs):
        ins = refs[: len(layout.arrays)]
        out_ref, x_ref, gate_ref, up_ref, sems = refs[len(layout.arrays) :]
        count = layout.count()
        (row_refs,) = layout.split(ins)
        waits = start_copies(layout.lists[0], row_refs, pos_ref, pos_ref[0], x_ref, sems, 0)
        gate_copy = pltpu.make_async_copy(gate_hbm, gate_ref, sems.at[count])
        up_copy = pltpu.make_async_copy(up_hbm, up_ref, sems.at[count + 1])
        gate_copy.start()
        up_copy.start()
        for w in waits:
            w.wait()
        normalise(x_ref, gain_ref)
        gate_copy.wait()
        gates = dot(gate_ref[...], x_ref[...], ((1,), (1,)))
        up_copy.wait()
        ups = dot(up_ref[...], x_ref[...], ((1,), (1,)))
        out_ref[...] = (silu(gates) * ups).astype(BF16)

    return pl.pallas_call(
        body,
        out_shape=jax.ShapeDtypeStruct((hidden, cap), BF16),
        in_specs=[SMEM_SPEC, VMEM_SPEC, HBM_SPEC, HBM_SPEC] + [HBM_SPEC] * len(layout.arrays),
        out_specs=VMEM_SPEC,
        scratch_shapes=[
            pltpu.VMEM((cap, features), BF16),
            pltpu.VMEM((hidden, features), BF16),
            pltpu.VMEM((hidden, features), BF16),
            pltpu.SemaphoreType.DMA((layout.count() + 2,)),
        ],
        name="expert_hidden",
    )(layout.positions(), gain, gate, up, *layout.arrays)


def expert_out(hidden_pieces, flag, down, gate_columns, chosen_lanes, bases, tok_dev):
    experts, hidden, width = down.shape
    cap = gate_columns.shape[0] // experts
    groups = len(bases)
    members = len(bases[0])
    layout = Layout(flag)
    layout.add(hidden_pieces)
    base_slot = len(layout.slots)
    for group in bases:
        layout.slots.extend(group)

    def body(pos_ref, gates_ref, chosen_ref, down_hbm, *refs):
        ins = refs[: len(layout.arrays)]
        outs = refs[len(layout.arrays) : len(layout.arrays) + groups]
        hidden_ref, down_ref, weighted_ref, sems = refs[len(layout.arrays) + groups :]
        (hidden_refs,) = layout.split(ins)
        waits = start_copies(
            layout.lists[0], hidden_refs, pos_ref, pos_ref[0], hidden_ref, sems, 0
        )
        down_copy = pltpu.make_async_copy(down_hbm, down_ref, sems.at[layout.count()])
        down_copy.start()
        down_copy.wait()
        for w in waits:
            w.wait()
        for expert in range(experts):
            rows = slice(expert * hidden, (expert + 1) * hidden)
            out = dot(hidden_ref[rows, :], down_ref[expert], ((0,), (0,)))
            own = slice(expert * cap, (expert + 1) * cap)
            weighted_ref[own, :] = (gates_ref[own, :] * out).astype(BF16)
        span = lax.broadcasted_iota(jnp.int32, (tok_dev, experts * cap), 0)
        for group in range(groups):
            for member in range(members):
                base = pos_ref[base_slot + group * members + member]
                picker = jnp.where(span == chosen_ref[...] - base, 1.0, 0.0).astype(BF16)
                placed = dot(picker, weighted_ref[...], ((1,), (0,)))
                outs[group][member] = placed.astype(BF16)

    return pl.pallas_call(
        body,
        out_shape=[jax.ShapeDtypeStruct((members, tok_dev, width), BF16)] * groups,
        in_specs=[SMEM_SPEC, VMEM_SPEC, VMEM_SPEC, HBM_SPEC]
        + [HBM_SPEC] * len(layout.arrays),
        out_specs=[VMEM_SPEC] * groups,
        scratch_shapes=[
            pltpu.VMEM((experts * hidden, cap), BF16),
            pltpu.VMEM((experts, hidden, width), BF16),
            pltpu.VMEM((experts * cap, width), BF16),
            pltpu.SemaphoreType.DMA((layout.count() + 1,)),
        ],
        name="expert_out",
    )(layout.positions(), gate_columns, chosen_lanes, down, *layout.arrays)


def shared_branch(token_pieces, gate_pieces, up_pieces, down_pieces, flag, gain, starts, width):
    tok_dev = token_pieces[0][0][0].shape[0]
    features = gain.shape[1]
    hidden = down_pieces[0][0][0].shape[0]
    layout = Layout(flag)
    for pieces in (token_pieces, gate_pieces, up_pieces, down_pieces):
        layout.add(pieces)
    start_slot = len(layout.slots)
    layout.slots.extend(starts)
    blocks = len(starts)

    def body(pos_ref, gain_ref, *refs):
        ins = refs[: len(layout.arrays)]
        outs = refs[len(layout.arrays) : len(layout.arrays) + blocks]
        x_ref, gate_ref, up_ref, down_ref, sum_ref, sems = refs[len(layout.arrays) + blocks :]
        flag_value = pos_ref[0]
        waits = []
        first = 0
        for entries, piece_refs, target in zip(
            layout.lists, layout.split(ins), (x_ref, gate_ref, up_ref, down_ref)
        ):
            waits.append(
                start_copies(entries, piece_refs, pos_ref, flag_value, target, sems, first)
            )
            first += len(entries)
        for w in waits[0]:
            w.wait()
        normalise(x_ref, gain_ref)
        for w in waits[1]:
            w.wait()
        gates = dot(x_ref[...], gate_ref[...], ((1,), (1,)))
        for w in waits[2]:
            w.wait()
        ups = dot(x_ref[...], up_ref[...], ((1,), (1,)))
        mid = (silu(gates) * ups).astype(BF16)
        for w in waits[3]:
            w.wait()
        sum_ref[...] = dot(mid, down_ref[...], ((1,), (0,)))
        for number in range(blocks):
            col = pl.multiple_of(pos_ref[start_slot + number], 128)
            outs[number][...] = sum_ref[:, pl.ds(col, width)].astype(outs[number].dtype)

    return pl.pallas_call(
        body,
        out_shape=[
            jax.ShapeDtypeStruct((tok_dev, width), F32 if n == 0 else BF16)
            for n in range(blocks)
        ],
        in_specs=[SMEM_SPEC, VMEM_SPEC] + [HBM_SPEC] * len(layout.arrays),
        out_specs=[VMEM_SPEC] * blocks,
        scratch_shapes=[
            pltpu.VMEM((tok_dev, features), BF16),
            pltpu.VMEM((hidden, features), BF16),
            pltpu.VMEM((hidden, features), BF16),
            pltpu.VMEM((hidden, features), BF16),
            pltpu.VMEM((tok_dev, features), F32),
            pltpu.SemaphoreType.DMA((layout.count(),)),
        ],
        name="shared_branch",
    )(layout.positions(), gain, *layout.arrays)


def on_device(
    tokens,
    norm_gain,
    shared_gate,
    shared_up,
    shared_down,
    expert_gate,
    expert_up,
    expert_down,
    chosen,
    gates,
):
    tp_count = lax.axis_size("tp")
    ep_count = lax.axis_size("ep")
    tp = lax.axis_index("tp").astype(jnp.int32)
    ep = lax.axis_index("ep").astype(jnp.int32)
    tok_dev, width = tokens.shape
    experts, cap = chosen.shape
    total = tok_dev * ep_count
    split = tp_count // experts
    own_expert = tp // split
    on_line = tp_count == 4 and experts == 2
    on_box = ep_count == 8
    flag = ((tp == 1) | (tp == 2)).astype(jnp.int32)
    gain = norm_gain[None, :]
    gate_weight = expert_gate.reshape(expert_gate.shape[2], expert_gate.shape[3])
    up_weight = expert_up.reshape(expert_up.shape[2], expert_up.shape[3])

    if on_box:
        source_pieces = [
            ([a], (ep ^ m) * tok_dev + h * (tok_dev // 2), None)
            for a, m, h in box_gather(tokens, "ep")
        ]
    else:
        source_pieces = [([lax.all_gather(tokens, "ep", axis=0, tiled=True)], None, None)]

    if on_line:
        token_pieces = [
            (a, None, (tp ^ m) * width) for a, m in line_gather(tokens, tokens, "tp")
        ]
    else:
        token_pieces = [([lax.all_gather(tokens, "tp", axis=1, tiled=True)], None, None)]

    def weight_pieces(weight):
        block = weight.shape[1]
        if on_box:
            half = weight.shape[0] // 2
            return [
                ([a], h * half, (ep ^ m) * block) for a, m, h in box_gather(weight, "ep")
            ]
        return [([lax.all_gather(weight, "ep", axis=1, tiled=True)], None, None)]

    gate_pieces = weight_pieces(shared_gate.T)
    up_pieces = weight_pieces(shared_up.T)
    down_pieces = weight_pieces(shared_down)

    if on_line:
        order = jnp.where(own_expert == 0, chosen, chosen[::-1])
        near, far = gather_rows(source_pieces, flag, order.reshape(-1, 1), total, cap)
        row_pieces = [(a, None, (tp ^ m) * width) for a, m in line_gather(near, far, "tp")]
    else:
        rows = gather_rows(source_pieces, flag, chosen.reshape(-1, 1), total, cap)
        copies = jnp.repeat(jnp.stack(rows), split, axis=0)
        joined = lax.all_to_all(copies, "tp", split_axis=0, concat_axis=2, tiled=True)
        row_pieces = [([joined.reshape(cap, -1)], None, None)]

    part_hidden = expert_hidden(row_pieces, flag, gain, gate_weight, up_weight)
    hidden_rows = part_hidden.shape[0]
    if on_line:
        hidden_pieces = [
            (a, (tp ^ m) * hidden_rows, None)
            for a, m in line_gather(part_hidden, part_hidden, "tp")
        ]
    else:
        hidden_pieces = [([lax.all_gather(part_hidden, "tp", axis=0, tiled=True)], None, None)]

    masks = range(tp_count) if on_line else None
    starts = [(tp ^ m) * width for m in range(4)] if on_line else [0]
    sums = shared_branch(
        token_pieces,
        gate_pieces,
        up_pieces,
        down_pieces,
        flag,
        gain,
        starts,
        width if on_line else width * tp_count,
    )
    if on_line:
        mixed = sums[0]
        for mask in range(1, 4):
            mixed = mixed + swap(sums[mask], "tp", mask).astype(F32)
    else:
        mixed = lax.psum_scatter(sums[0], "tp", scatter_dimension=1, tiled=True)

    if on_box:
        bases = [[(ep ^ m ^ p) * tok_dev for m in (0, 2, 4, 6)] for p in (1, 0)]
    else:
        bases = [[i * tok_dev for i in range(ep_count)]]
    placed = expert_out(
        hidden_pieces,
        flag,
        expert_down,
        gates.reshape(-1, 1),
        chosen.reshape(1, -1),
        bases,
        tok_dev,
    )
    if on_box:
        both = placed[1].astype(F32) + swap(placed[0], "ep", 1).astype(F32)
        mixed = mixed + both[0]
        for number, mask in ((1, 2), (2, 4), (3, 6)):
            mixed = mixed + swap(both[number].astype(BF16), "ep", mask).astype(F32)
    else:
        flat = placed[0].reshape(total, width).astype(F32)
        mixed = mixed + lax.psum_scatter(flat, "ep", scatter_dimension=0, tiled=True)
    return mixed.astype(BF16)


def solution(mesh):
    return jax.shard_map(
        on_device,
        mesh=mesh,
        in_specs=(
            P("ep", "tp"),
            P(),
            P("ep", "tp"),
            P("ep", "tp"),
            P("tp", "ep"),
            P("tp", "ep", None, None),
            P("tp", "ep", None, None),
            P("ep", None, "tp"),
            P("ep", None),
            P("ep", None),
        ),
        out_specs=P("ep", "tp"),
        check_vma=False,
    )
```

```python
import jax
import jax.numpy as jnp
from jax import lax
from jax.experimental import pallas as pl
from jax.experimental.pallas import tpu as pltpu
from jax.sharding import PartitionSpec as P


norm_eps = 1e-06
F32 = jnp.float32
BF16 = jnp.bfloat16
MIB = 1 << 20


VMEM_SPEC = pl.BlockSpec(memory_space=pltpu.VMEM)
SMEM_SPEC = pl.BlockSpec(memory_space=pltpu.SMEM)
HBM_SPEC = pl.BlockSpec(memory_space=pltpu.HBM)


def swap(x, axis, mask):
    count = lax.axis_size(axis)
    return lax.ppermute(x, axis, [(i, i ^ mask) for i in range(count)])


def line_gather(near, far, axis):
    pair = lax.ppermute(near, axis, [(0, 1), (1, 0), (2, 3), (3, 2)])
    middle = lax.ppermute(far, axis, [(1, 2), (2, 1)])
    ends = lax.ppermute(far, axis, [(0, 2), (3, 1)])
    relay_middle = lax.ppermute(middle, axis, [(2, 3), (1, 0)])
    outer = lax.ppermute(far, axis, [(0, 3), (3, 0)])
    return [
        ([near], 0),
        ([pair], 1),
        ([ends, relay_middle], 2),
        ([middle, outer], 3),
    ]


def line_scatter(blocks, axis):
    one, two, three = blocks
    middle = lax.ppermute(three, axis, [(1, 2), (2, 1)])
    inward = lax.ppermute(two, axis, [(0, 2), (3, 1)])
    pair = swap(one, axis, 1)
    outward = lax.ppermute(two, axis, [(2, 0), (1, 3)])
    ends = lax.ppermute(three, axis, [(0, 3), (3, 0)])
    return [([pair], 1), ([inward, outward], 2), ([middle, ends], 3)]


def box_gather(x, axis, relay):
    near = {2: swap(x, axis, 2), 4: swap(x, axis, 4)}
    diagonal = swap(near.get(6 - relay, x), axis, relay)
    pieces = [(x, 0), (near[2], 2), (near[4], 4)]
    pieces += [(swap(a, axis, 1), m ^ 1) for a, m in pieces]
    pieces += [(diagonal, 6), (swap(diagonal, axis, 1), 7)]
    return [([a], m) for a, m in pieces]


def arrays_of(pieces):
    return [a for arrays, _ in pieces for a in arrays]


def read_piece(arrays, refs, at, flag):
    if len(arrays) == 1:
        return refs[at][...]
    return jnp.where(flag != 0, refs[at][...], refs[at + 1][...])


def copy_pieces(pieces, refs, flag, pos_ref, slot, target, dim):
    at = 0
    for number, (arrays, _) in enumerate(pieces):
        value = read_piece(arrays, refs, at, flag)
        at += len(arrays)
        if len(pieces) == 1:
            target[...] = value
        elif dim == 0:
            row = pl.multiple_of(pos_ref[slot + number], 64)
            target[pl.ds(row, value.shape[0]), :] = value
        else:
            col = pl.multiple_of(pos_ref[slot + number], 128)
            target[:, pl.ds(col, value.shape[1])] = value


def stack_scalars(values):
    return jnp.stack([jnp.asarray(v, jnp.int32) for v in values])


def silu(v):
    return v / (1.0 + jnp.exp(-v))


def normalise(x_ref, gain_ref):
    wide = x_ref[...].astype(F32)
    scale = lax.rsqrt(jnp.mean(wide * wide, axis=1, keepdims=True) + norm_eps)
    x_ref[...] = (wide * scale * gain_ref[...]).astype(BF16)


def dot(a, b, dims):
    return lax.dot_general(a, b, (dims, ((), ())), preferred_element_type=F32)


def one_hot(ids, shape, dim):
    span = lax.broadcasted_iota(jnp.int32, shape, dim)
    return jnp.where(ids == span, 1.0, 0.0).astype(BF16)


def kernel(body, out_shape, in_specs, scratch_shapes):
    outs = len(out_shape) if isinstance(out_shape, list) else None
    return pl.pallas_call(
        body,
        out_shape=out_shape,
        in_specs=in_specs,
        out_specs=VMEM_SPEC if outs is None else [VMEM_SPEC] * outs,
        scratch_shapes=scratch_shapes,
        compiler_params=pltpu.CompilerParams(vmem_limit_bytes=60 * MIB),
    )


def take_windows(pieces, flag, ids_column):
    arrays = arrays_of(pieces)
    tok_dev, width = arrays[0].shape
    slots = ids_column.shape[0]

    def body(pos_ref, ids_ref, *refs):
        picker = one_hot(ids_ref[...], (slots, tok_dev), 1)
        at = 0
        for number, (alternatives, _) in enumerate(pieces):
            value = read_piece(alternatives, refs, at, pos_ref[0])
            at += len(alternatives)
            rows = dot(picker, value, ((1,), (0,))).astype(BF16)
            refs[-1][:, number * width : (number + 1) * width] = rows

    return kernel(
        body,
        jax.ShapeDtypeStruct((slots, width * len(pieces)), BF16),
        [SMEM_SPEC] + [VMEM_SPEC] * (1 + len(arrays)),
        [],
    )(flag, ids_column, *arrays)


def expert_hidden(windows, width, positions, slot_lanes, gain, gate, up, cap):
    hidden, features = gate.shape

    def body(pos_ref, slot_ref, gain_ref, gate_hbm, up_hbm, *refs):
        out_ref, x_ref, gate_ref, up_ref, sems = refs[len(windows) :]
        gate_copy = pltpu.make_async_copy(gate_hbm, gate_ref, sems.at[0])
        up_copy = pltpu.make_async_copy(up_hbm, up_ref, sems.at[1])
        gate_copy.start()
        up_copy.start()
        picker = one_hot(slot_ref[...], (cap, slot_ref.shape[1]), 0)
        for number in range(len(windows)):
            rows = dot(picker, refs[number][...], ((1,), (0,))).astype(BF16)
            for part in range(rows.shape[1] // width):
                at = 1 + number * (rows.shape[1] // width) + part
                col = pl.multiple_of(pos_ref[at], 128)
                x_ref[:, pl.ds(col, width)] = rows[:, part * width : (part + 1) * width]
        normalise(x_ref, gain_ref)
        gate_copy.wait()
        gates = dot(gate_ref[...], x_ref[...], ((1,), (1,)))
        up_copy.wait()
        ups = dot(up_ref[...], x_ref[...], ((1,), (1,)))
        out_ref[...] = (silu(gates) * ups).astype(BF16)

    return kernel(
        body,
        jax.ShapeDtypeStruct((hidden, cap), BF16),
        [SMEM_SPEC, VMEM_SPEC, VMEM_SPEC, HBM_SPEC, HBM_SPEC] + [VMEM_SPEC] * len(windows),
        [
            pltpu.VMEM((cap, features), BF16),
            pltpu.VMEM((hidden, features), BF16),
            pltpu.VMEM((hidden, features), BF16),
            pltpu.SemaphoreType.DMA((2,)),
        ],
    )(positions, slot_lanes, gain, gate, up, *windows)


def expert_down(hidden_pieces, positions, down, gate_column, slot_rows):
    hidden, width = down.shape
    cap = gate_column.shape[0]
    slots = slot_rows.shape[0]
    arrays = arrays_of(hidden_pieces)

    def body(pos_ref, gate_ref, slot_ref, down_ref, *refs):
        out_ref, hidden_ref = refs[len(arrays) :]
        copy_pieces(hidden_pieces, refs, pos_ref[0], pos_ref, 1, hidden_ref, 0)
        out = dot(hidden_ref[...], down_ref[...], ((0,), (0,)))
        weighted = (gate_ref[...] * out).astype(BF16)
        picker = one_hot(slot_ref[...], (slots, cap), 1)
        out_ref[...] = dot(picker, weighted, ((1,), (0,))).astype(BF16)

    return kernel(
        body,
        jax.ShapeDtypeStruct((slots, width), BF16),
        [SMEM_SPEC] + [VMEM_SPEC] * (3 + len(arrays)),
        [pltpu.VMEM((hidden, cap), BF16)],
    )(positions, gate_column, slot_rows, down, *arrays)


def add_products(x_ref, total_ref, weights, positions, first):
    for number, (weight, col) in enumerate(zip(weights, positions)):
        x = x_ref[:, pl.ds(pl.multiple_of(col, 128), weight.shape[1])]
        part = dot(x, weight[...], ((1,), (1,)))
        if first and number == 0:
            total_ref[...] = part
        else:
            total_ref[...] += part


def shared_in(token_pieces, gates, ups, positions, gain):
    token_arrays = arrays_of(token_pieces)
    gate_arrays, up_arrays = arrays_of(gates), arrays_of(ups)
    tok_dev = token_arrays[0].shape[0]
    features = gain.shape[1]
    hidden = gate_arrays[0].shape[0]
    ends = [len(token_arrays), len(token_arrays) + len(gate_arrays)]
    count = ends[1] + len(up_arrays)

    def body(pos_ref, gain_ref, *refs):
        x_ref, gate_sum, up_sum = refs[count:]
        copy_pieces(token_pieces, refs, pos_ref[0], pos_ref, 1, x_ref, 1)
        normalise(x_ref, gain_ref)
        at = [pos_ref[1 + n] for n in range(count)]
        add_products(x_ref, gate_sum, refs[ends[0] : ends[1]], at[ends[0] : ends[1]], True)
        add_products(x_ref, up_sum, refs[ends[1] : count], at[ends[1] :], True)

    return kernel(
        body,
        [
            jax.ShapeDtypeStruct((tok_dev, features), BF16),
            jax.ShapeDtypeStruct((tok_dev, hidden), F32),
            jax.ShapeDtypeStruct((tok_dev, hidden), F32),
        ],
        [SMEM_SPEC] + [VMEM_SPEC] * (1 + count),
        [],
    )(positions, gain, *token_arrays, *gate_arrays, *up_arrays)


def shared_out(begun, gates, ups, downs, positions, width, blocks):
    arrays = arrays_of(gates) + arrays_of(ups) + arrays_of(downs)
    ends = [len(gates), len(gates) + len(ups)]
    count = len(arrays)
    tok_dev, features = begun[0].shape
    hidden = begun[1].shape[1]
    block = arrays[-1].shape[1]

    def body(pos_ref, x_ref, gate_in, up_in, *refs):
        outs = refs[count : count + blocks]
        gate_sum, up_sum, sum_ref = refs[count + blocks :]
        at = [pos_ref[n] for n in range(count)]
        gate_sum[...] = gate_in[...]
        add_products(x_ref, gate_sum, refs[: ends[0]], at[: ends[0]], False)
        up_sum[...] = up_in[...]
        add_products(x_ref, up_sum, refs[ends[0] : ends[1]], at[ends[0] : ends[1]], False)
        mid = (silu(gate_sum[...]) * up_sum[...]).astype(BF16)
        for number in range(ends[1], count):
            col = pl.multiple_of(at[number], 128)
            sum_ref[:, pl.ds(col, block)] = dot(mid, refs[number][...], ((1,), (0,)))
        for number in range(blocks):
            col = pl.multiple_of(pos_ref[count + number], 128)
            outs[number][...] = sum_ref[:, pl.ds(col, width)].astype(outs[number].dtype)

    return kernel(
        body,
        [
            jax.ShapeDtypeStruct((tok_dev, width), F32 if n == 0 else BF16)
            for n in range(blocks)
        ],
        [SMEM_SPEC] + [VMEM_SPEC] * (3 + count),
        [
            pltpu.VMEM((tok_dev, hidden), F32),
            pltpu.VMEM((tok_dev, hidden), F32),
            pltpu.VMEM((tok_dev, features), F32),
        ],
    )(positions, *begun, *arrays)


def finish(shared_own, shared_parts, windows, ids, flag, tok_dev):
    width = shared_own.shape[1]
    arrays = arrays_of(shared_parts)
    parts = len(arrays)

    def body(pos_ref, own_ref, *refs):
        total = own_ref[...]
        at = 0
        for alternatives, _ in shared_parts:
            total = total + read_piece(alternatives, refs, at, pos_ref[0]).astype(F32)
            at += len(alternatives)
        for number in range(len(windows)):
            values, id_ref = refs[parts + number], refs[parts + len(windows) + number]
            picker = one_hot(id_ref[...], (tok_dev, values.shape[0]), 0)
            total = total + dot(picker, values[...], ((1,), (0,)))
        refs[-1][...] = total.astype(BF16)

    return kernel(
        body,
        jax.ShapeDtypeStruct((tok_dev, width), BF16),
        [SMEM_SPEC] + [VMEM_SPEC] * (1 + parts + 2 * len(windows)),
        [],
    )(flag, shared_own, *arrays, *windows, *ids)


def on_device(
    tokens,
    norm_gain,
    shared_gate,
    shared_up,
    shared_down,
    expert_gate,
    expert_up,
    expert_down_weight,
    chosen,
    gates,
):
    tp_count = lax.axis_size("tp")
    ep_count = lax.axis_size("ep")
    tp = lax.axis_index("tp").astype(jnp.int32)
    ep = lax.axis_index("ep").astype(jnp.int32)
    tok_dev, width = tokens.shape
    experts, cap = chosen.shape
    split = tp_count // experts
    on_line = tp_count == 4 and experts == 2
    on_box = ep_count == 8
    inner = ((tp == 1) | (tp == 2)).astype(jnp.int32)
    gain = norm_gain[None, :]
    gate_weight = expert_gate.reshape(expert_gate.shape[2], expert_gate.shape[3])
    up_weight = expert_up.reshape(expert_up.shape[2], expert_up.shape[3])

    own_expert = tp // split
    order = [own_expert, 1 - own_expert]
    chosen_of = [lax.dynamic_index_in_dim(chosen, k, 0, keepdims=False) for k in order]
    gates_of = [lax.dynamic_index_in_dim(gates, k, 0, keepdims=False) for k in order]
    down_of = [
        lax.dynamic_index_in_dim(expert_down_weight, k, 0, keepdims=False) for k in order
    ]

    if on_line:
        token_pieces = [([tokens], 0)]
        token_pieces += [([swap(tokens, "tp", m)], m) for m in (1, 2, 3)]
    else:
        token_pieces = [([lax.all_gather(tokens, "tp", axis=1, tiled=True)], 0)]

    def gathered(weight, relay):
        if on_box:
            return box_gather(weight, "ep", relay)
        return [([lax.all_gather(weight, "ep", axis=1, tiled=True)], 0)]

    block = shared_down.shape[1]
    shared_gates = gathered(shared_gate.T, 2)
    shared_ups = gathered(shared_up.T, 6)
    shared_downs = gathered(shared_down, 4)

    window = 2 * cap // ep_count
    owner_start = jnp.arange(ep_count, dtype=jnp.int32) * tok_dev
    offsets = jnp.arange(window, dtype=jnp.int32)
    slot_rows = []
    slot_ids = []
    for ids in chosen_of:
        starts = jnp.sum((ids[None, :] < owner_start[:, None]).astype(jnp.int32), axis=1)
        rows = (starts[:, None] + offsets[None, :]).reshape(-1)
        slot_rows.append(rows.reshape(-1, 1))
        hit = rows[:, None] == jnp.arange(cap, dtype=jnp.int32)[None, :]
        found = jnp.sum(jnp.where(hit, ids[None, :] + 1, 0), axis=1) - 1
        slot_ids.append(found.reshape(ep_count, window) - owner_start[:, None])
    sent_ids = jnp.stack(slot_ids, axis=1)
    owner_ids = lax.all_to_all(sent_ids, "ep", split_axis=0, concat_axis=0, tiled=True)
    owner_ids = [owner_ids[:, k].reshape(1, -1) for k in range(experts)]

    feature_at = [inner] + [(tp ^ m) * width for _, m in token_pieces]
    flag = stack_scalars([inner])
    ids_column = owner_ids[0].reshape(-1, 1)
    arrived = []
    arrived_at = [inner]
    for number in range(0, len(token_pieces), 2):
        batch = token_pieces[number : number + 2]
        sent = take_windows(batch, flag, ids_column)
        sent = sent.reshape(ep_count, window, -1)
        rows = lax.all_to_all(sent, "ep", split_axis=0, concat_axis=0, tiled=True)
        arrived.append(rows.reshape(ep_count * window, -1))
        arrived_at += [(tp ^ mask) * width for _, mask in batch]
    piece_width = width if on_line else width * tp_count
    if not on_line:
        arrived_at = [inner, 0]
    part_hidden = expert_hidden(
        arrived,
        piece_width,
        stack_scalars(arrived_at),
        slot_rows[0].reshape(1, -1),
        gain,
        gate_weight,
        up_weight,
        cap,
    )

    hidden_rows = part_hidden.shape[0]
    if on_line:
        pieces = line_gather(part_hidden, part_hidden, "tp")
        hidden_of = [pieces[:2], pieces[2:]]
    else:
        whole = lax.all_gather(part_hidden, "tp", axis=0, tiled=True)
        units = hidden_rows * split
        hidden_of = [
            [([lax.dynamic_slice_in_dim(whole, k * units, units, 0)], 0)] for k in order
        ]

    def places(pieces):
        return [(ep ^ m) * block if on_box else 0 for _, m in pieces]

    early_gates, early_ups = shared_gates[:6], shared_ups[:6]
    late_gates, late_ups = shared_gates[6:], shared_ups[6:]
    in_at = feature_at + places(early_gates + early_ups)
    begun = shared_in(token_pieces, early_gates, early_ups, stack_scalars(in_at), gain)
    masks = [0, 1, 2, 3] if on_line else [0]
    out_at = places(late_gates + late_ups + shared_downs)
    out_at += [(tp ^ m) * width for m in masks] if on_line else [0]
    sums = shared_out(
        begun,
        late_gates,
        late_ups,
        shared_downs,
        stack_scalars(out_at),
        width if on_line else width * tp_count,
        len(masks),
    )
    if on_line:
        shared_own = sums[0]
        shared_parts = line_scatter(sums[1:], "tp")
    else:
        shared_own = lax.psum_scatter(sums[0], "tp", scatter_dimension=1, tiled=True)
        shared_parts = []

    windows = []
    for k in range(experts):
        hidden_at = [inner] + [((tp ^ m) % split) * hidden_rows for _, m in hidden_of[k]]
        sent = expert_down(
            hidden_of[k],
            stack_scalars(hidden_at),
            down_of[k],
            gates_of[k].reshape(-1, 1),
            slot_rows[k],
        )
        windows.append(lax.all_to_all(sent, "ep", split_axis=0, concat_axis=0, tiled=True))
    return finish(shared_own, shared_parts, windows, owner_ids, flag, tok_dev)


def solution(mesh):
    return jax.shard_map(
        on_device,
        mesh=mesh,
        in_specs=(
            P("ep", "tp"),
            P(),
            P("ep", "tp"),
            P("ep", "tp"),
            P("tp", "ep"),
            P("tp", "ep", None, None),
            P("tp", "ep", None, None),
            P("ep", None, "tp"),
            P("ep", None),
            P("ep", None),
        ),
        out_specs=P("ep", "tp"),
        check_vma=False,
    )
```

```python
import jax
import jax.numpy as jnp
from jax import lax
from jax.experimental import pallas as pl
from jax.experimental.pallas import tpu as pltpu
from jax.sharding import PartitionSpec as P


norm_eps = 1e-06
F32 = jnp.float32
BF16 = jnp.bfloat16
MIB = 1 << 20


VMEM_SPEC = pl.BlockSpec(memory_space=pltpu.VMEM)
SMEM_SPEC = pl.BlockSpec(memory_space=pltpu.SMEM)
HBM_SPEC = pl.BlockSpec(memory_space=pltpu.HBM)


def swap(x, axis, mask):
    count = lax.axis_size(axis)
    return lax.ppermute(x, axis, [(i, i ^ mask) for i in range(count)])


def direct_gather(near, far, axis):
    pieces = [([near], 0)]
    for mask, x in ((1, near), (2, far), (3, far)):
        pieces.append(([swap(x, axis, mask)], mask))
    return pieces


def box_gather(x, axis, relay):
    near = {2: swap(x, axis, 2), 4: swap(x, axis, 4)}
    diagonal = swap(near.get(6 - relay, x), axis, relay)
    pieces = [(x, 0), (near[2], 2), (near[4], 4)]
    pieces += [(swap(a, axis, 1), m ^ 1) for a, m in pieces]
    pieces += [(diagonal, 6), (swap(diagonal, axis, 1), 7)]
    return [([a], m) for a, m in pieces]


def arrays_of(pieces):
    return [a for arrays, _ in pieces for a in arrays]


def read_piece(arrays, refs, at, flag):
    if len(arrays) == 1:
        return refs[at][...]
    return jnp.where(flag != 0, refs[at][...], refs[at + 1][...])


def copy_pieces(pieces, refs, flag, pos_ref, slot, target, dim):
    at = 0
    for number, (arrays, _) in enumerate(pieces):
        value = read_piece(arrays, refs, at, flag)
        at += len(arrays)
        if len(pieces) == 1:
            target[...] = value
        elif dim == 0:
            row = pl.multiple_of(pos_ref[slot + number], 64)
            target[pl.ds(row, value.shape[0]), :] = value
        else:
            col = pl.multiple_of(pos_ref[slot + number], 128)
            target[:, pl.ds(col, value.shape[1])] = value


def stack_scalars(values):
    return jnp.stack([jnp.asarray(v, jnp.int32) for v in values])


def silu(v):
    return v / (1.0 + jnp.exp(-v))


def normalise(x_ref, gain_ref):
    wide = x_ref[...].astype(F32)
    scale = lax.rsqrt(jnp.mean(wide * wide, axis=1, keepdims=True) + norm_eps)
    x_ref[...] = (wide * scale * gain_ref[...]).astype(BF16)


def dot(a, b, dims):
    return lax.dot_general(a, b, (dims, ((), ())), preferred_element_type=F32)


def one_hot(ids, shape, dim):
    span = lax.broadcasted_iota(jnp.int32, shape, dim)
    return jnp.where(ids == span, 1.0, 0.0).astype(BF16)


def as_column(row):
    return jnp.transpose(jnp.broadcast_to(row, (8, row.shape[1])))[:, :1]


def kernel(body, out_shape, in_specs, scratch_shapes, mib):
    outs = len(out_shape) if isinstance(out_shape, list) else None
    return pl.pallas_call(
        body,
        out_shape=out_shape,
        in_specs=in_specs,
        out_specs=VMEM_SPEC if outs is None else [VMEM_SPEC] * outs,
        scratch_shapes=scratch_shapes,
        compiler_params=pltpu.CompilerParams(vmem_limit_bytes=mib * MIB),
    )


def take_windows(pieces, flag, ids_lanes):
    arrays = arrays_of(pieces)
    tok_dev, width = arrays[0].shape
    slots = ids_lanes.shape[1]

    def body(pos_ref, ids_ref, *refs):
        picker = one_hot(as_column(ids_ref[...]), (slots, tok_dev), 1)
        at = 0
        for number, (alternatives, _) in enumerate(pieces):
            value = read_piece(alternatives, refs, at, pos_ref[0])
            at += len(alternatives)
            rows = dot(picker, value, ((1,), (0,))).astype(BF16)
            refs[-1][:, number * width : (number + 1) * width] = rows

    return kernel(
        body,
        jax.ShapeDtypeStruct((slots, width * len(pieces)), BF16),
        [SMEM_SPEC] + [VMEM_SPEC] * (1 + len(arrays)),
        [],
        60,
    )(flag, ids_lanes, *arrays)


def as_row(column):
    return jnp.transpose(jnp.broadcast_to(column, (column.shape[0], 128)))[:1, :]


def expert_hidden(window, width, positions, slot_lanes, gain, gate, up, cap, begun, last):
    hidden, features = gate.shape
    parts = window.shape[1] // width
    prior = 3 if begun else 0

    def body(pos_ref, slot_ref, gain_ref, gate_hbm, up_hbm, window_ref, *refs):
        outs = refs[prior:-4]
        gate_ref, up_ref, x_ref, sems = refs[-4:]
        cols = [pl.multiple_of(pos_ref[n], 128) for n in range(parts)]
        copies = []
        for matrix, (source, target) in enumerate(((gate_hbm, gate_ref), (up_hbm, up_ref))):
            for n, col in enumerate(cols):
                copy = pltpu.make_async_copy(
                    source.at[:, pl.ds(col, width)],
                    target.at[:, pl.ds(n * width, width)],
                    sems.at[matrix * parts + n],
                )
                copy.start()
                copies.append(copy)
        picker = one_hot(slot_ref[...], (cap, slot_ref.shape[1]), 0)
        rows = dot(picker, window_ref[...], ((1,), (0,)))
        squares = as_row(jnp.sum(rows * rows, axis=1, keepdims=True))
        for n, col in enumerate(cols):
            span = slice(n * width, (n + 1) * width)
            x_ref[:, span] = (rows[:, span] * gain_ref[:, pl.ds(col, width)]).astype(BF16)
        for copy in copies[:parts]:
            copy.wait()
        gates = dot(gate_ref[...], x_ref[...], ((1,), (1,)))
        for copy in copies[parts:]:
            copy.wait()
        ups = dot(up_ref[...], x_ref[...], ((1,), (1,)))
        if begun:
            gates = gates + refs[0][...]
            ups = ups + refs[1][...]
            squares = squares + refs[2][...]
        if last:
            scale = lax.rsqrt(squares * (1.0 / features) + norm_eps)
            outs[0][...] = (silu(gates * scale) * (ups * scale)).astype(BF16)
        else:
            outs[0][...] = gates
            outs[1][...] = ups
            outs[2][...] = squares

    products = jax.ShapeDtypeStruct((hidden, cap), F32)
    result = [jax.ShapeDtypeStruct((hidden, cap), BF16)]
    if not last:
        result = [products, products, jax.ShapeDtypeStruct((1, cap), F32)]
    return kernel(
        body,
        result,
        [SMEM_SPEC, VMEM_SPEC, VMEM_SPEC] + [HBM_SPEC] * 2 + [VMEM_SPEC] * (1 + prior),
        [
            pltpu.VMEM((hidden, parts * width), BF16),
            pltpu.VMEM((hidden, parts * width), BF16),
            pltpu.VMEM((cap, parts * width), BF16),
            pltpu.SemaphoreType.DMA((2 * parts,)),
        ],
        56,
    )(positions, slot_lanes, gain, gate, up, window, *(begun or []))


def expert_down(hidden_pieces, positions, downs, gate_lanes, slot_lanes):
    _, hidden, width = downs.shape
    cap = gate_lanes.shape[1]
    slots = slot_lanes.shape[1]
    arrays = arrays_of(hidden_pieces)

    def body(pos_ref, gate_ref, slot_ref, down_hbm, *refs):
        out_ref, hidden_ref, down_ref, sem = refs[len(arrays) :]
        expert = pos_ref[1 + len(hidden_pieces)]
        copy = pltpu.make_async_copy(down_hbm.at[expert], down_ref, sem)
        copy.start()
        copy_pieces(hidden_pieces, refs, pos_ref[0], pos_ref, 1, hidden_ref, 0)
        picker = one_hot(as_column(slot_ref[...]), (slots, cap), 1)
        gate = as_column(gate_ref[...])
        copy.wait()
        out = dot(hidden_ref[...], down_ref[...], ((0,), (0,)))
        weighted = (gate * out).astype(BF16)
        out_ref[...] = dot(picker, weighted, ((1,), (0,))).astype(BF16)

    return kernel(
        body,
        jax.ShapeDtypeStruct((slots, width), BF16),
        [SMEM_SPEC, VMEM_SPEC, VMEM_SPEC, HBM_SPEC] + [VMEM_SPEC] * len(arrays),
        [
            pltpu.VMEM((hidden, cap), BF16),
            pltpu.VMEM((hidden, width), BF16),
            pltpu.SemaphoreType.DMA(()),
        ],
        60,
    )(positions, gate_lanes, slot_lanes, downs, *arrays)


def add_products(x_ref, total_ref, weights, positions, first):
    for number, (weight, col) in enumerate(zip(weights, positions)):
        x = x_ref[:, pl.ds(pl.multiple_of(col, 128), weight.shape[1])]
        part = dot(x, weight[...], ((1,), (1,)))
        if first and number == 0:
            total_ref[...] = part
        else:
            total_ref[...] += part


def shared_in(token_pieces, gates, ups, positions, gain):
    token_arrays = arrays_of(token_pieces)
    gate_arrays, up_arrays = arrays_of(gates), arrays_of(ups)
    tok_dev = token_arrays[0].shape[0]
    features = gain.shape[1]
    hidden = gate_arrays[0].shape[0]
    ends = [len(token_arrays), len(token_arrays) + len(gate_arrays)]
    count = ends[1] + len(up_arrays)

    def body(pos_ref, gain_ref, *refs):
        x_ref, gate_sum, up_sum = refs[count:]
        copy_pieces(token_pieces, refs, pos_ref[0], pos_ref, 1, x_ref, 1)
        normalise(x_ref, gain_ref)
        first = 1 + len(token_pieces)
        at = [pos_ref[first + n] for n in range(len(gate_arrays) + len(up_arrays))]
        add_products(x_ref, gate_sum, refs[ends[0] : ends[1]], at[: len(gate_arrays)], True)
        add_products(x_ref, up_sum, refs[ends[1] : count], at[len(gate_arrays) :], True)

    return kernel(
        body,
        [
            jax.ShapeDtypeStruct((tok_dev, features), BF16),
            jax.ShapeDtypeStruct((tok_dev, hidden), F32),
            jax.ShapeDtypeStruct((tok_dev, hidden), F32),
        ],
        [SMEM_SPEC] + [VMEM_SPEC] * (1 + count),
        [],
        60,
    )(positions, gain, *token_arrays, *gate_arrays, *up_arrays)


def shared_out(begun, gates, ups, downs, positions, width, blocks):
    arrays = arrays_of(gates) + arrays_of(ups) + arrays_of(downs)
    ends = [len(gates), len(gates) + len(ups)]
    count = len(arrays)
    tok_dev, features = begun[0].shape
    hidden = begun[1].shape[1]
    block = arrays[-1].shape[1]

    def body(pos_ref, x_ref, gate_in, up_in, *refs):
        outs = refs[count:-3]
        gate_sum, up_sum, sum_ref = refs[-3:]
        at = [pos_ref[n] for n in range(count)]
        gate_sum[...] = gate_in[...]
        add_products(x_ref, gate_sum, refs[: ends[0]], at[: ends[0]], False)
        up_sum[...] = up_in[...]
        add_products(x_ref, up_sum, refs[ends[0] : ends[1]], at[ends[0] : ends[1]], False)
        mid = (silu(gate_sum[...]) * up_sum[...]).astype(BF16)
        for number in range(ends[1], count):
            col = pl.multiple_of(at[number], 128)
            sum_ref[:, pl.ds(col, block)] = dot(mid, refs[number][...], ((1,), (0,)))
        for number in range(blocks):
            col = pl.multiple_of(pos_ref[count + number], 128)
            block_sum = sum_ref[:, pl.ds(col, width)]
            if number < 2:
                outs[number][...] = block_sum
            else:
                rows = slice((number - 2) * tok_dev, (number - 1) * tok_dev)
                outs[2][rows, :] = block_sum.astype(BF16)

    return kernel(
        body,
        [jax.ShapeDtypeStruct((tok_dev, width), F32)] * min(blocks, 2)
        + [jax.ShapeDtypeStruct(((blocks - 2) * tok_dev, width), BF16)] * (blocks > 2),
        [SMEM_SPEC] + [VMEM_SPEC] * (3 + count),
        [
            pltpu.VMEM((tok_dev, hidden), F32),
            pltpu.VMEM((tok_dev, hidden), F32),
            pltpu.VMEM((tok_dev, features), F32),
        ],
        60,
    )(positions, *begun, *arrays)


def finish(shared_own, shared_parts, windows, ids, tok_dev):
    width = shared_own.shape[1]
    parts = len(shared_parts)

    def body(own_ref, *refs):
        total = own_ref[...]
        for number in range(parts):
            total = total + refs[number][:tok_dev, :].astype(F32)
        for number in range(len(windows)):
            values, id_ref = refs[parts + number], refs[parts + len(windows) + number]
            picker = one_hot(id_ref[...], (tok_dev, values.shape[0]), 0)
            total = total + dot(picker, values[...], ((1,), (0,)))
        refs[-1][...] = total.astype(BF16)

    return kernel(
        body,
        jax.ShapeDtypeStruct((tok_dev, width), BF16),
        [VMEM_SPEC] * (1 + parts + 2 * len(windows)),
        [],
        54,
    )(shared_own, *shared_parts, *windows, *ids)


def on_device(
    tokens,
    norm_gain,
    shared_gate,
    shared_up,
    shared_down,
    expert_gate,
    expert_up,
    expert_down_weight,
    chosen,
    gates,
):
    tp_count = lax.axis_size("tp")
    ep_count = lax.axis_size("ep")
    tp = lax.axis_index("tp").astype(jnp.int32)
    ep = lax.axis_index("ep").astype(jnp.int32)
    tok_dev, width = tokens.shape
    experts, cap = chosen.shape
    split = tp_count // experts
    on_line = tp_count == 4 and experts == 2
    on_box = ep_count == 8
    inner = ((tp == 1) | (tp == 2)).astype(jnp.int32)
    gain = norm_gain[None, :]
    gate_weight = expert_gate.reshape(expert_gate.shape[2], expert_gate.shape[3])
    up_weight = expert_up.reshape(expert_up.shape[2], expert_up.shape[3])

    own_expert = tp // split
    order = [own_expert, 1 - own_expert]
    chosen_of = [lax.dynamic_index_in_dim(chosen, k, 0, keepdims=False) for k in order]
    gates_of = [lax.dynamic_index_in_dim(gates, k, 0, keepdims=False) for k in order]

    if on_line:
        token_pieces = direct_gather(tokens, tokens, "tp")
    else:
        token_pieces = [([lax.all_gather(tokens, "tp", axis=1, tiled=True)], 0)]

    def gathered(weight, relay):
        if on_box:
            return box_gather(weight, "ep", relay)
        return [([lax.all_gather(weight, "ep", axis=1, tiled=True)], 0)]

    block = shared_down.shape[1]
    shared_gates = gathered(shared_gate.T, 2)
    shared_ups = gathered(shared_up.T, 6)
    shared_downs = gathered(shared_down, 4)

    window = 2 * cap // ep_count
    owner_start = jnp.arange(ep_count, dtype=jnp.int32) * tok_dev
    offsets = jnp.arange(window, dtype=jnp.int32)
    slot_rows = []
    slot_ids = []
    for ids in chosen_of:
        starts = jnp.sum((ids[None, :] < owner_start[:, None]).astype(jnp.int32), axis=1)
        rows = (starts[:, None] + offsets[None, :]).reshape(-1)
        slot_rows.append(rows.reshape(1, -1))
        hit = rows[:, None] == jnp.arange(cap, dtype=jnp.int32)[None, :]
        found = jnp.sum(jnp.where(hit, ids[None, :] + 1, 0), axis=1) - 1
        slot_ids.append(found.reshape(ep_count, window) - owner_start[:, None])
    sent_ids = jnp.stack(slot_ids, axis=1)
    owner_ids = lax.all_to_all(sent_ids, "ep", split_axis=0, concat_axis=0, tiled=True)
    owner_ids = [owner_ids[:, k].reshape(1, -1) for k in range(experts)]

    feature_at = [inner] + [(tp ^ m) * width for _, m in token_pieces]
    flag = stack_scalars([inner])
    begun = None
    for number in range(0, len(token_pieces), 2):
        batch = token_pieces[number : number + 2]
        sent = take_windows(batch, flag, owner_ids[0])
        sent = sent.reshape(ep_count, window, -1)
        rows = lax.all_to_all(sent, "ep", split_axis=0, concat_axis=0, tiled=True)
        begun = expert_hidden(
            rows.reshape(ep_count * window, -1),
            width if on_line else width * tp_count,
            stack_scalars([(tp ^ m) * width if on_line else 0 for _, m in batch]),
            slot_rows[0],
            gain,
            gate_weight,
            up_weight,
            cap,
            begun,
            number + 2 >= len(token_pieces),
        )
    part_hidden = begun[0]

    hidden_rows = part_hidden.shape[0]
    if on_line:
        pieces = direct_gather(part_hidden, part_hidden, "tp")
        hidden_of = [pieces[:2], pieces[2:]]
    else:
        whole = lax.all_gather(part_hidden, "tp", axis=0, tiled=True)
        units = hidden_rows * split
        hidden_of = [
            [([lax.dynamic_slice_in_dim(whole, k * units, units, 0)], 0)] for k in order
        ]

    def places(pieces):
        return [(ep ^ m) * block if on_box else 0 for _, m in pieces]

    early_gates, early_ups = shared_gates[:6], shared_ups[:6]
    late_gates, late_ups = shared_gates[6:], shared_ups[6:]
    in_at = feature_at + places(early_gates + early_ups)
    shared_begun = shared_in(token_pieces, early_gates, early_ups, stack_scalars(in_at), gain)
    masks = [0, 2, 1, 3] if on_line else [0]
    out_at = places(late_gates + late_ups + shared_downs)
    out_at += [(tp ^ m) * width for m in masks] if on_line else [0]
    sums = shared_out(
        shared_begun,
        late_gates,
        late_ups,
        shared_downs,
        stack_scalars(out_at),
        width if on_line else width * tp_count,
        len(masks),
    )
    if on_line:
        near = swap(sums[2], "tp", 1)
        half = (sums[1] + near[tok_dev:].astype(F32)).astype(BF16)
        shared_own = sums[0]
        shared_parts = [near, swap(half, "tp", 2)]
    else:
        shared_own = lax.psum_scatter(sums[0], "tp", scatter_dimension=1, tiled=True)
        shared_parts = []

    windows = []
    for k in range(experts):
        hidden_at = [inner] + [((tp ^ m) % split) * hidden_rows for _, m in hidden_of[k]]
        sent = expert_down(
            hidden_of[k],
            stack_scalars(hidden_at + [order[k]]),
            expert_down_weight,
            gates_of[k].reshape(1, -1),
            slot_rows[k],
        )
        sent = sent.reshape(ep_count, window, width)
        rows = lax.all_to_all(sent, "ep", split_axis=0, concat_axis=0, tiled=True)
        windows.append(rows.reshape(ep_count * window, width))
    return finish(shared_own, shared_parts, windows, owner_ids, tok_dev)


def solution(mesh):
    return jax.shard_map(
        on_device,
        mesh=mesh,
        in_specs=(
            P("ep", "tp"),
            P(),
            P("ep", "tp"),
            P("ep", "tp"),
            P("tp", "ep"),
            P("tp", "ep", None, None),
            P("tp", "ep", None, None),
            P("ep", None, "tp"),
            P("ep", None),
            P("ep", None),
        ),
        out_specs=P("ep", "tp"),
        check_vma=False,
    )
```

```python
import jax
import jax.numpy as jnp
from jax import lax
from jax.experimental import pallas as pl
from jax.experimental.pallas import tpu as pltpu
from jax.sharding import PartitionSpec as P


norm_eps = 1e-06
F32 = jnp.float32
BF16 = jnp.bfloat16
MIB = 1 << 20


VMEM_SPEC = pl.BlockSpec(memory_space=pltpu.VMEM)
SMEM_SPEC = pl.BlockSpec(memory_space=pltpu.SMEM)
HBM_SPEC = pl.BlockSpec(memory_space=pltpu.HBM)


def swap(x, axis, mask):
    count = lax.axis_size(axis)
    return lax.ppermute(x, axis, [(i, i ^ mask) for i in range(count)])


def direct_gather(near, far, axis):
    pieces = [([near], 0)]
    for mask, x in ((1, near), (2, far), (3, far)):
        pieces.append(([swap(x, axis, mask)], mask))
    return pieces


def box_gather(x, axis, relay):
    near = {2: swap(x, axis, 2), 4: swap(x, axis, 4)}
    diagonal = swap(near.get(6 - relay, x), axis, relay)
    pieces = [(x, 0), (near[2], 2), (near[4], 4)]
    pieces += [(swap(a, axis, 1), m ^ 1) for a, m in pieces]
    pieces += [(diagonal, 6), (swap(diagonal, axis, 1), 7)]
    return [([a], m) for a, m in pieces]


def arrays_of(pieces):
    return [a for arrays, _ in pieces for a in arrays]


def read_piece(arrays, refs, at, flag):
    if len(arrays) == 1:
        return refs[at][...]
    return jnp.where(flag != 0, refs[at][...], refs[at + 1][...])


def copy_pieces(pieces, refs, flag, pos_ref, slot, target, dim):
    at = 0
    for number, (arrays, _) in enumerate(pieces):
        value = read_piece(arrays, refs, at, flag)
        at += len(arrays)
        if len(pieces) == 1:
            target[...] = value
        elif dim == 0:
            row = pl.multiple_of(pos_ref[slot + number], 64)
            target[pl.ds(row, value.shape[0]), :] = value
        else:
            col = pl.multiple_of(pos_ref[slot + number], 128)
            target[:, pl.ds(col, value.shape[1])] = value


def stack_scalars(values):
    return jnp.stack([jnp.asarray(v, jnp.int32) for v in values])


def silu(v):
    return v / (1.0 + jnp.exp(-v))


def normalise(x_ref, gain_ref):
    wide = x_ref[...].astype(F32)
    scale = lax.rsqrt(jnp.mean(wide * wide, axis=1, keepdims=True) + norm_eps)
    x_ref[...] = (wide * scale * gain_ref[...]).astype(BF16)


def dot(a, b, dims):
    return lax.dot_general(a, b, (dims, ((), ())), preferred_element_type=F32)


def one_hot(ids, shape, dim):
    span = lax.broadcasted_iota(jnp.int32, shape, dim)
    return jnp.where(ids == span, 1.0, 0.0).astype(BF16)


def as_column(row):
    return jnp.transpose(jnp.broadcast_to(row, (8, row.shape[1])))[:, :1]


def kernel(body, out_shape, in_specs, scratch_shapes, mib):
    outs = len(out_shape) if isinstance(out_shape, list) else None
    return pl.pallas_call(
        body,
        out_shape=out_shape,
        in_specs=in_specs,
        out_specs=VMEM_SPEC if outs is None else [VMEM_SPEC] * outs,
        scratch_shapes=scratch_shapes,
        compiler_params=pltpu.CompilerParams(vmem_limit_bytes=mib * MIB),
    )


def take_windows(pieces, flag, ids_lanes):
    arrays = arrays_of(pieces)
    tok_dev, width = arrays[0].shape
    slots = ids_lanes.shape[1]

    def body(pos_ref, ids_ref, *refs):
        picker = one_hot(as_column(ids_ref[...]), (slots, tok_dev), 1)
        at = 0
        for number, (alternatives, _) in enumerate(pieces):
            value = read_piece(alternatives, refs, at, pos_ref[0])
            at += len(alternatives)
            rows = dot(picker, value, ((1,), (0,))).astype(BF16)
            refs[-1][:, number * width : (number + 1) * width] = rows

    return kernel(
        body,
        jax.ShapeDtypeStruct((slots, width * len(pieces)), BF16),
        [SMEM_SPEC] + [VMEM_SPEC] * (1 + len(arrays)),
        [],
        60,
    )(flag, ids_lanes, *arrays)


def as_row(column):
    return jnp.transpose(jnp.broadcast_to(column, (column.shape[0], 128)))[:1, :]


def expert_hidden(window, width, positions, slot_lanes, gain, gate, up, cap, begun, last):
    hidden, features = gate.shape
    parts = window.shape[1] // width
    prior = 3 if begun else 0

    def body(pos_ref, slot_ref, gain_ref, gate_hbm, up_hbm, window_ref, *refs):
        outs = refs[prior : prior + len(result)]
        gate_ref, up_ref, x_ref, sems, *sums = refs[prior + len(result) :]
        sum_copies = [
            pltpu.make_async_copy(refs[n], sums[n], sems.at[2 * parts + n])
            for n in range(len(sums))
        ]
        cols = [pl.multiple_of(pos_ref[n], 128) for n in range(parts)]
        copies = []
        for matrix, (source, target) in enumerate(((gate_hbm, gate_ref), (up_hbm, up_ref))):
            for n, col in enumerate(cols):
                copy = pltpu.make_async_copy(
                    source.at[:, pl.ds(col, width)],
                    target.at[:, pl.ds(n * width, width)],
                    sems.at[matrix * parts + n],
                )
                copy.start()
                copies.append(copy)
        for copy in sum_copies:
            copy.start()
        picker = one_hot(slot_ref[...], (cap, slot_ref.shape[1]), 0)
        rows = dot(picker, window_ref[...], ((1,), (0,)))
        squares = as_row(jnp.sum(rows * rows, axis=1, keepdims=True))
        for n, col in enumerate(cols):
            span = slice(n * width, (n + 1) * width)
            x_ref[:, span] = (rows[:, span] * gain_ref[:, pl.ds(col, width)]).astype(BF16)
        for copy in copies[:parts]:
            copy.wait()
        gates = dot(gate_ref[...], x_ref[...], ((1,), (1,)))
        for copy in copies[parts:]:
            copy.wait()
        ups = dot(up_ref[...], x_ref[...], ((1,), (1,)))
        if begun:
            for copy in sum_copies:
                copy.wait()
            gates = gates + sums[0][...]
            ups = ups + sums[1][...]
            squares = squares + refs[2][...]
        if last:
            scale = lax.rsqrt(squares * (1.0 / features) + norm_eps)
            outs[0][...] = (silu(gates * scale) * (ups * scale)).astype(BF16)
        else:
            outs[0][...] = gates
            outs[1][...] = ups
            outs[2][...] = squares

    products = jax.ShapeDtypeStruct((hidden, cap), F32)
    result = [jax.ShapeDtypeStruct((hidden, cap), BF16)]
    if not last:
        result = [products, products, jax.ShapeDtypeStruct((1, cap), F32)]
    return kernel(
        body,
        result,
        [SMEM_SPEC, VMEM_SPEC, VMEM_SPEC] + [HBM_SPEC] * 2 + [VMEM_SPEC] + ([HBM_SPEC] * 2 + [VMEM_SPEC]) * (prior > 0),
        [
            pltpu.VMEM((hidden, parts * width), BF16),
            pltpu.VMEM((hidden, parts * width), BF16),
            pltpu.VMEM((cap, parts * width), BF16),
            pltpu.SemaphoreType.DMA((2 * parts + 2,)),
        ]
        + [pltpu.VMEM((hidden, cap), F32)] * (2 if begun else 0),
        56,
    )(positions, slot_lanes, gain, gate, up, window, *(begun or []))


def expert_down(hidden_pieces, positions, downs, gate_lanes, slot_lanes):
    _, hidden, width = downs.shape
    cap = gate_lanes.shape[1]
    slots = slot_lanes.shape[1]
    arrays = arrays_of(hidden_pieces)

    def body(pos_ref, gate_ref, slot_ref, down_hbm, *refs):
        out_ref, hidden_ref, down_ref, sem = refs[len(arrays) :]
        expert = pos_ref[1 + len(hidden_pieces)]
        copy = pltpu.make_async_copy(down_hbm.at[expert], down_ref, sem)
        copy.start()
        copy_pieces(hidden_pieces, refs, pos_ref[0], pos_ref, 1, hidden_ref, 0)
        picker = one_hot(as_column(slot_ref[...]), (slots, cap), 1)
        gate = as_column(gate_ref[...])
        copy.wait()
        out = dot(hidden_ref[...], down_ref[...], ((0,), (0,)))
        weighted = (gate * out).astype(BF16)
        out_ref[...] = dot(picker, weighted, ((1,), (0,))).astype(BF16)

    return kernel(
        body,
        jax.ShapeDtypeStruct((slots, width), BF16),
        [SMEM_SPEC, VMEM_SPEC, VMEM_SPEC, HBM_SPEC] + [VMEM_SPEC] * len(arrays),
        [
            pltpu.VMEM((hidden, cap), BF16),
            pltpu.VMEM((hidden, width), BF16),
            pltpu.SemaphoreType.DMA(()),
        ],
        60,
    )(positions, gate_lanes, slot_lanes, downs, *arrays)


def add_products(x_ref, total_ref, weights, positions, first):
    for number, (weight, col) in enumerate(zip(weights, positions)):
        x = x_ref[:, pl.ds(pl.multiple_of(col, 128), weight.shape[1])]
        part = dot(x, weight[...], ((1,), (1,)))
        if first and number == 0:
            total_ref[...] = part
        else:
            total_ref[...] += part


def shared_in(token_pieces, gates, ups, positions, gain):
    token_arrays = arrays_of(token_pieces)
    gate_arrays, up_arrays = arrays_of(gates), arrays_of(ups)
    tok_dev = token_arrays[0].shape[0]
    features = gain.shape[1]
    hidden = gate_arrays[0].shape[0]
    ends = [len(token_arrays), len(token_arrays) + len(gate_arrays)]
    count = ends[1] + len(up_arrays)

    def body(pos_ref, gain_ref, *refs):
        x_ref, gate_sum, up_sum = refs[count:]
        copy_pieces(token_pieces, refs, pos_ref[0], pos_ref, 1, x_ref, 1)
        normalise(x_ref, gain_ref)
        first = 1 + len(token_pieces)
        at = [pos_ref[first + n] for n in range(len(gate_arrays) + len(up_arrays))]
        add_products(x_ref, gate_sum, refs[ends[0] : ends[1]], at[: len(gate_arrays)], True)
        add_products(x_ref, up_sum, refs[ends[1] : count], at[len(gate_arrays) :], True)

    return kernel(
        body,
        [
            jax.ShapeDtypeStruct((tok_dev, features), BF16),
            jax.ShapeDtypeStruct((tok_dev, hidden), F32),
            jax.ShapeDtypeStruct((tok_dev, hidden), F32),
        ],
        [SMEM_SPEC] + [VMEM_SPEC] * (1 + count),
        [],
        60,
    )(positions, gain, *token_arrays, *gate_arrays, *up_arrays)


def shared_out(begun, gates, ups, downs, positions, width, blocks):
    arrays = arrays_of(gates) + arrays_of(ups) + arrays_of(downs)
    ends = [len(gates), len(gates) + len(ups)]
    count = len(arrays)
    tok_dev, features = begun[0].shape
    hidden = begun[1].shape[1]
    block = arrays[-1].shape[1]

    def body(pos_ref, x_ref, gate_in, up_in, *refs):
        outs = refs[count:-3]
        gate_sum, up_sum, sum_ref = refs[-3:]
        at = [pos_ref[n] for n in range(count)]
        gate_sum[...] = gate_in[...]
        add_products(x_ref, gate_sum, refs[: ends[0]], at[: ends[0]], False)
        up_sum[...] = up_in[...]
        add_products(x_ref, up_sum, refs[ends[0] : ends[1]], at[ends[0] : ends[1]], False)
        mid = (silu(gate_sum[...]) * up_sum[...]).astype(BF16)
        for number in range(ends[1], count):
            col = pl.multiple_of(at[number], 128)
            sum_ref[:, pl.ds(col, block)] = dot(mid, refs[number][...], ((1,), (0,)))
        for number in range(blocks):
            col = pl.multiple_of(pos_ref[count + number], 128)
            outs[number][...] = sum_ref[:, pl.ds(col, width)].astype(outs[number].dtype)

    return kernel(
        body,
        [
            jax.ShapeDtypeStruct((tok_dev, width), F32 if n < 2 else BF16)
            for n in range(blocks)
        ],
        [SMEM_SPEC] + [VMEM_SPEC] * (3 + count),
        [
            pltpu.VMEM((tok_dev, hidden), F32),
            pltpu.VMEM((tok_dev, hidden), F32),
            pltpu.VMEM((tok_dev, features), F32),
        ],
        60,
    )(positions, *begun, *arrays)


def finish(shared_own, shared_parts, windows, ids, tok_dev, dtype):
    width = shared_own.shape[1]
    parts = len(shared_parts)

    def body(own_ref, *refs):
        total = own_ref[...]
        for number in range(parts):
            total = total + refs[number][...].astype(F32)
        for number in range(len(windows)):
            values, id_ref = refs[parts + number], refs[parts + len(windows) + number]
            picker = one_hot(id_ref[...], (tok_dev, values.shape[0]), 0)
            total = total + dot(picker, values[...], ((1,), (0,)))
        refs[-1][...] = total.astype(dtype)

    return kernel(
        body,
        jax.ShapeDtypeStruct((tok_dev, width), dtype),
        [VMEM_SPEC] * (1 + parts + 2 * len(windows)),
        [],
        54,
    )(shared_own, *shared_parts, *windows, *ids)


def on_device(
    tokens,
    norm_gain,
    shared_gate,
    shared_up,
    shared_down,
    expert_gate,
    expert_up,
    expert_down_weight,
    chosen,
    gates,
):
    tp_count = lax.axis_size("tp")
    ep_count = lax.axis_size("ep")
    tp = lax.axis_index("tp").astype(jnp.int32)
    ep = lax.axis_index("ep").astype(jnp.int32)
    tok_dev, width = tokens.shape
    experts, cap = chosen.shape
    split = tp_count // experts
    on_line = tp_count == 4 and experts == 2
    on_box = ep_count == 8
    inner = ((tp == 1) | (tp == 2)).astype(jnp.int32)
    gain = norm_gain[None, :]
    gate_weight = expert_gate.reshape(expert_gate.shape[2], expert_gate.shape[3])
    up_weight = expert_up.reshape(expert_up.shape[2], expert_up.shape[3])

    own_expert = tp // split
    order = [own_expert, 1 - own_expert]
    chosen_of = [lax.dynamic_index_in_dim(chosen, k, 0, keepdims=False) for k in order]
    gates_of = [lax.dynamic_index_in_dim(gates, k, 0, keepdims=False) for k in order]

    if on_line:
        token_pieces = direct_gather(tokens, tokens, "tp")
    else:
        token_pieces = [([lax.all_gather(tokens, "tp", axis=1, tiled=True)], 0)]

    def gathered(weight, relay):
        if on_box:
            return box_gather(weight, "ep", relay)
        return [([lax.all_gather(weight, "ep", axis=1, tiled=True)], 0)]

    block = shared_down.shape[1]
    shared_gates = gathered(shared_gate.T, 2)
    shared_ups = gathered(shared_up.T, 6)
    shared_downs = gathered(shared_down, 4)

    window = 2 * cap // ep_count
    owner_start = jnp.arange(ep_count, dtype=jnp.int32) * tok_dev
    offsets = jnp.arange(window, dtype=jnp.int32)
    slot_rows = []
    slot_ids = []
    for ids in chosen_of:
        starts = jnp.sum((ids[None, :] < owner_start[:, None]).astype(jnp.int32), axis=1)
        rows = (starts[:, None] + offsets[None, :]).reshape(-1)
        slot_rows.append(rows.reshape(1, -1))
        hit = rows[:, None] == jnp.arange(cap, dtype=jnp.int32)[None, :]
        found = jnp.sum(jnp.where(hit, ids[None, :] + 1, 0), axis=1) - 1
        slot_ids.append(found.reshape(ep_count, window) - owner_start[:, None])
    sent_ids = jnp.stack(slot_ids, axis=1)
    owner_ids = lax.all_to_all(sent_ids, "ep", split_axis=0, concat_axis=0, tiled=True)
    owner_ids = [owner_ids[:, k].reshape(1, -1) for k in range(experts)]

    feature_at = [inner] + [(tp ^ m) * width for _, m in token_pieces]
    flag = stack_scalars([inner])
    begun = None
    for number in range(0, len(token_pieces), 2):
        batch = token_pieces[number : number + 2]
        sent = take_windows(batch, flag, owner_ids[0])
        sent = sent.reshape(ep_count, window, -1)
        rows = lax.all_to_all(sent, "ep", split_axis=0, concat_axis=0, tiled=True)
        begun = expert_hidden(
            rows.reshape(ep_count * window, -1),
            width if on_line else width * tp_count,
            stack_scalars([(tp ^ m) * width if on_line else 0 for _, m in batch]),
            slot_rows[0],
            gain,
            gate_weight,
            up_weight,
            cap,
            begun,
            number + 2 >= len(token_pieces),
        )
    part_hidden = begun[0]

    hidden_rows = part_hidden.shape[0]
    if on_line:
        pieces = direct_gather(part_hidden, part_hidden, "tp")
        hidden_of = [pieces[:2], pieces[2:]]
    else:
        whole = lax.all_gather(part_hidden, "tp", axis=0, tiled=True)
        units = hidden_rows * split
        hidden_of = [
            [([lax.dynamic_slice_in_dim(whole, k * units, units, 0)], 0)] for k in order
        ]

    def places(pieces):
        return [(ep ^ m) * block if on_box else 0 for _, m in pieces]

    early_gates, early_ups = shared_gates[:6], shared_ups[:6]
    late_gates, late_ups = shared_gates[6:], shared_ups[6:]
    in_at = feature_at + places(early_gates + early_ups)
    shared_begun = shared_in(token_pieces, early_gates, early_ups, stack_scalars(in_at), gain)
    masks = [0, 2, 3, 1] if on_line else [0]
    out_at = places(late_gates + late_ups + shared_downs)
    out_at += [(tp ^ m) * width for m in masks] if on_line else [0]
    sums = shared_out(
        shared_begun,
        late_gates,
        late_ups,
        shared_downs,
        stack_scalars(out_at),
        width if on_line else width * tp_count,
        len(masks),
    )
    if on_line:
        near = swap(sums[2], "tp", 1)
        half = (sums[1] + near.astype(F32)).astype(BF16)
        shared_own = sums[0]
        shared_parts = [swap(sums[3], "tp", 1), swap(half, "tp", 2)]
    else:
        shared_own = lax.psum_scatter(sums[0], "tp", scatter_dimension=1, tiled=True)
        shared_parts = []

    windows = []
    for k in range(experts):
        hidden_at = [inner] + [((tp ^ m) % split) * hidden_rows for _, m in hidden_of[k]]
        sent = expert_down(
            hidden_of[k],
            stack_scalars(hidden_at + [order[k]]),
            expert_down_weight,
            gates_of[k].reshape(1, -1),
            slot_rows[k],
        )
        sent = sent.reshape(ep_count, window, width)
        rows = lax.all_to_all(sent, "ep", split_axis=0, concat_axis=0, tiled=True)
        windows.append(rows.reshape(ep_count * window, width))
    first = finish(shared_own, [], windows[:1], owner_ids[:1], tok_dev, F32)
    return finish(first, shared_parts, windows[1:], owner_ids[1:], tok_dev, BF16)


def solution(mesh):
    return jax.shard_map(
        on_device,
        mesh=mesh,
        in_specs=(
            P("ep", "tp"),
            P(),
            P("ep", "tp"),
            P("ep", "tp"),
            P("tp", "ep"),
            P("tp", "ep", None, None),
            P("tp", "ep", None, None),
            P("ep", None, "tp"),
            P("ep", None),
            P("ep", None),
        ),
        out_specs=P("ep", "tp"),
        check_vma=False,
    )
```
